32 devices in a mesh: row: 8 (over z, y), col: 4 (over x, core).
Axes of the slice: x: 2, y: 2, z: 4, core: 2. Of those that a mesh axis runs over, the one named last changes fastest.
Arguments:
- tracer: float32 [128, 128, 512], P(None, 'row', 'col'), may hold values from -6 to 6
- symbol_x: float32 [128], replicated, may hold values from 0.3 to 3
- symbol_y: float32 [128], replicated, may hold values from 0.3 to 3
- symbol_z: float32 [512], replicated, may hold values from 0.3 to 3
Outputs:
- spectrum: float32 [128, 128, 512], P('row', 'col')
The draws below stay inside these ranges and needn't reach their ends.
All inputs are finite; a program needn't handle non-finite values.
Results may differ from the reference program's by a relative error of at most 0.000075.
Values sent between devices are 32-bit elements; how exact they have to be, the bound alone decides.
A program may use at most 64 MiB of HBM per device.

```python
import jax
import jax.numpy as jnp
from jax import lax

GRID_X = 128
GRID_Y = 128
GRID_Z = 512


def level_of(stream_key, extent, shards, smallest, largest):
    def one(axis_at, shards_of):
        draws = jax.random.uniform(jax.random.fold_in(jax.random.fold_in(stream_key, 6), axis_at), (shards_of,), jnp.float32, smallest / len(shards), largest / len(shards))
        return jnp.repeat(jnp.exp(draws), extent[axis_at] // shards_of).reshape((-1,) + (1,) * (len(extent) - axis_at - 1))

    level = one(*shards[0])
    for cut in shards[1:]:
        level = level * one(*cut)
    return level


def gaussian(key, dims, deviation, most, cuts=(), dtype=jnp.bfloat16):
    loudness = level_of(key, dims, cuts, -0.22, 0.18) if cuts else 1.0
    values = jax.random.normal(key, dims, jnp.float32) * deviation * loudness
    return jnp.minimum(jnp.maximum(values, -most), most).astype(dtype)


def setup_inputs(seed: int = 0) -> dict:
    seeds = jax.random.split(jax.random.key(seed), 5)
    return {
        "tracer": gaussian(seeds[0], (GRID_X, GRID_Y, GRID_Z), 1.0, 6.0, ((1, 8), (2, 4)), jnp.float32),
        "symbol_x": jnp.clip(jax.random.uniform(seeds[1], (GRID_X,), jnp.float32, 0.3, 3.0), 0.3, 3.0),
        "symbol_y": jnp.clip(jax.random.uniform(seeds[2], (GRID_Y,), jnp.float32, 0.3, 3.0), 0.3, 3.0),
        "symbol_z": jnp.clip(jax.random.uniform(seeds[3], (GRID_Z,), jnp.float32, 0.3, 3.0), 0.3, 3.0),
    }


def transform_table(count):
    rank = jnp.arange(count)
    angle = (jnp.pi / (count + 1)) * (((rank[:, None] + 1) * (rank[None, :] + 1)) % (2 * count + 2)).astype(jnp.float32)
    return jnp.sin(angle) * (2.0 / (count + 1)) ** 0.5


def to_modes(values, dim):
    moved = jnp.tensordot(values, transform_table(values.shape[dim]), axes=([dim], [0]), precision=lax.Precision.HIGHEST)
    return jnp.moveaxis(moved, -1, dim)


def reference(tracer, symbol_x, symbol_y, symbol_z):
    spectrum = tracer
    spectrum = to_modes(spectrum, 0)
    spectrum = to_modes(spectrum, 1)
    spectrum = to_modes(spectrum, 2)
    symbol = symbol_x[:, None, None] + symbol_y[None, :, None] + symbol_z[None, None, :]
    spectrum = spectrum * ((1.0 - 0.2 * symbol) / (1.0 + 0.2 * symbol))
    return spectrum
```

```python
import functools

import jax
import jax.numpy as jnp
import ml_dtypes
import numpy as np
from jax import lax
from jax.experimental import pallas as pl
from jax.experimental.pallas import tpu as pltpu
from jax.sharding import PartitionSpec as P

MESH = pl.DeviceIdType.MESH
F32 = jnp.float32
BF16 = jnp.bfloat16
LAG = 1


def table_halves(count):
    rank = np.arange(1, count + 1)
    turns = np.outer(rank, rank) % (2 * count + 2)
    table = np.sin(np.pi / (count + 1) * turns) * np.sqrt(2.0 / (count + 1))
    high = table.astype(ml_dtypes.bfloat16)
    low = (table - high.astype(np.float64)).astype(ml_dtypes.bfloat16)
    return high, low


def left_table(high, low):
    return np.concatenate(
        [np.concatenate([high, high], axis=1), np.concatenate([low, 0 * low], axis=1)]
    )


def halves(values):
    high = values.astype(BF16)
    return high, (values - high.astype(F32)).astype(BF16)


def dot(a, b):
    return jnp.dot(a, b, preferred_element_type=F32)


def from_left(table, values):
    rows = table.shape[0] // 2
    both = dot(table, jnp.concatenate(halves(values), axis=0))
    return both[:rows] + both[rows:]


def piece_sizes(share):
    size = max(1, share // 4)
    sizes = []
    left = share
    while left:
        size = min(size, left)
        if left <= size:
            size = max(1, left // 2)
        sizes.append(size)
        left -= size
    return sizes


def kernel(
    n, m, sizes, groups, block,
    field, tab_x, tab_y, tab_zh, tab_zl, sx, sy, sz, out,
    d, s, r, y, c, f, tx, ty, tzh, tzl, colx, coly, vx, vy, vz,
    in_sem, send_r, recv_r, send_c, recv_c, up_r, up_c,
):
    pieces = len(sizes)
    starts = [sum(sizes[:k]) for k in range(pieces)]
    lag = min(LAG, pieces)
    me_r, me_c = lax.axis_index("row"), lax.axis_index("col")
    depth, ys, zs = d.shape
    yc = y.shape[1]
    loads = [(field, d, 0), (tab_x, tx, 1), (tab_y, ty, 2), (tab_zh, tzh, 3), (tab_zl, tzl, 4)]
    loads += [(sx, vx, 5), (sy, vy, 6), (sz, vz, 7)]
    loads = [pltpu.make_async_copy(a, b, in_sem.at[i]) for a, b, i in loads]

    odd = lax.rem(me_r, 2)
    tier = lax.div(me_r, 2)
    tiers = n // 2
    barrier = pltpu.get_barrier_semaphore()
    flip = 1 if m % 2 == 0 else 0
    place = lambda at: at ^ flip

    def greet_row(to, _):
        @pl.when(jnp.logical_or(odd == 0, lax.rem(to, 2) == 1))
        def _():
            pl.semaphore_signal(barrier, inc=1, device_id={"row": to}, device_id_type=MESH)

        return 0

    def greet_col(at, _):
        pl.semaphore_signal(barrier, inc=1, device_id={"col": place(at)}, device_id_type=MESH)
        return 0

    lax.fori_loop(me_r + 1, n, greet_row, 0)
    lax.fori_loop(place(me_c) + 1, m, greet_col, 0)
    for load in loads:
        load.start()
    earlier = jnp.where(odd == 1, me_r, tier) + place(me_c)

    @pl.when(earlier > 0)
    def _():
        pl.semaphore_wait(barrier, earlier)

    @pl.when(odd == 1)
    def _():
        def answer(to, _):
            pl.semaphore_signal(
                up_r.at[tier], inc=1, device_id={"row": to}, device_id_type=MESH
            )
            return 0

        lax.fori_loop(0, me_r, answer, 0)

    def answer_col(at, _):
        pl.semaphore_signal(up_c, inc=1, device_id={"col": place(at)}, device_id_type=MESH)
        return 0

    lax.fori_loop(0, place(me_c), answer_col, 0)

    loads[0].wait()
    loads[1].wait()
    lanes = d.reshape(depth * ys, zs)
    modes = s.reshape(s.shape[0] * ys, zs)

    def transform_x(first, count):
        begin = n * starts[first]
        rows = n * sum(sizes[first : first + count])
        table = tx[2 * begin : 2 * (begin + rows)]

        def pair(i, _):
            got = jnp.concatenate(
                [lanes[pl.ds(2 * i + h, depth, stride=ys), :] for h in range(2)], axis=1
            )
            got = from_left(table, got)
            for h in range(2):
                modes[pl.ds(begin * ys + 2 * i + h, rows, stride=ys), :] = got[
                    :, h * zs : (h + 1) * zs
                ]
            return 0

        lax.fori_loop(0, ys // 2, pair, 0, unroll=True)

    mine = pl.ds(pl.multiple_of(me_r * ys, ys), ys)

    def send_row(k, to):
        each = sizes[k]
        pltpu.make_async_remote_copy(
            src_ref=s.at[pl.ds(n * starts[k] + to * each, each)],
            dst_ref=r.at[pl.ds(starts[k], each), mine, :],
            send_sem=send_r.at[k],
            recv_sem=recv_r.at[k],
            device_id={"row": to},
            device_id_type=MESH,
        ).start()

    def keep_row(k):
        each = sizes[k]
        r[pl.ds(starts[k], each), mine, :] = s[pl.ds(n * starts[k] + me_r * each, each)]

    def send_rows(k):
        def one(i, _):
            send_row(k, lax.rem(me_r + 1 + i, n))
            return 0

        lax.fori_loop(0, n - 1, one, 0)
        keep_row(k)

    def wait_up(at):
        pl.semaphore_wait(up_r.at[at], 1)

    def first_rows(k):
        @pl.when(odd == 0)
        def _():
            wait_up(tier)

        def low(to, _):
            @pl.when(to != me_r)
            def _():
                send_row(k, to)

            return 0

        lax.fori_loop(0, 2 * tier + 2, low, 0)

    def later_rows(k):
        def late(at, _):
            wait_up(at)
            for h in range(2):
                send_row(k, 2 * at + h)
            return 0

        lax.fori_loop(tier + 1, tiers, late, 0)
        keep_row(k)

    for at, (first, count) in enumerate(groups):
        transform_x(first, count)
        if at == 0:
            first_rows(0)
        if at == min(1, len(groups) - 1):
            later_rows(0)
        for k in range(max(1, first), first + count):
            send_rows(k)

    for load in loads[2:]:
        load.wait()

    def upright(row_ref, into):
        size = row_ref.shape[1]
        here = lax.broadcasted_iota(jnp.int32, (size, size), 0)
        there = lax.broadcasted_iota(jnp.int32, (size, size), 1)
        kept = jnp.where(here == there, row_ref[...], 0.0)
        into[...] = jnp.broadcast_to(jnp.sum(kept, axis=1, keepdims=True), into.shape)

    upright(vx, colx)
    upright(vy, coly)
    x_share = r.shape[0]
    part_y = coly[pl.ds(pl.multiple_of(me_c * yc, yc), yc), :]

    def factor(i, _):
        symbol = part_y + colx[pl.ds(me_r * x_share + i, 1), :]
        for at in range(0, vz.shape[1], 128):
            full = symbol + vz[:, at : at + 128]
            f[pl.ds(pl.multiple_of(i * yc, yc), yc), at : at + 128] = (1.0 - 0.2 * full) / (
                1.0 + 0.2 * full
            )
        return 0

    lax.fori_loop(0, x_share, factor, 0)

    @pl.when(place(me_c) < m - 1)
    def _():
        pl.semaphore_wait(up_c, m - 1 - place(me_c))

    def got_rows(k):
        waited = r.at[pl.ds(starts[k], sizes[k]), pl.ds(0, (n - 1) * ys), :]
        pltpu.make_async_copy(waited, waited, recv_r.at[k]).wait()

    def transform_y(k):
        each, base = sizes[k], m * starts[k]
        got = jnp.concatenate([r[starts[k] + j] for j in range(each)], axis=1)
        for b in range(ty.shape[0] // (2 * block)):
            now = from_left(ty[2 * b * block : 2 * (b + 1) * block], got)
            for q in range(block // yc):
                for j in range(each):
                    y[base + (b * (block // yc) + q) * each + j] = now[
                        q * yc : (q + 1) * yc, j * zs : (j + 1) * zs
                    ]

    def send_cols(k):
        each, base = sizes[k], m * starts[k]

        def one(i, _):
            to = lax.rem(me_c + i, m)
            pltpu.make_async_remote_copy(
                src_ref=y.at[pl.ds(base + to * each, each)],
                dst_ref=c.at[pl.ds(base + me_c * each, each)],
                send_sem=send_c.at[k],
                recv_sem=recv_c.at[k],
                device_id={"col": to},
                device_id_type=MESH,
            ).start()
            return 0

        lax.fori_loop(1, m, one, 0)
        own = pl.ds(base + me_c * each, each)
        c[own] = y[own]

    def got_cols(k):
        waited = c.at[pl.ds(m * starts[k], (m - 1) * sizes[k])]
        pltpu.make_async_copy(waited, waited, recv_c.at[k]).wait()

    def transform_z(k):
        each, base = sizes[k], m * starts[k]
        rows = each * yc
        got = jnp.concatenate(
            [c[base + q * each : base + (q + 1) * each].reshape(rows, zs) for q in range(m)],
            axis=1,
        )
        high, low = halves(got)
        both = dot(jnp.concatenate([high, low], axis=0), tzh[...])
        full = both[:rows] + both[rows:] + dot(high, tzl[...])
        at = slice(starts[k] * yc, starts[k] * yc + rows)
        out[at, :] = full * f[at, :]

    for k in range(pieces):
        got_rows(k)
        transform_y(k)
        send_cols(k)
        if k >= lag:
            got_cols(k - lag)
            transform_z(k - lag)
    for k in range(pieces - lag, pieces):
        got_cols(k)
        transform_z(k)

    for k in range(pieces):
        sent = s.at[pl.ds(0, (n - 1) * sizes[k])]
        pltpu.make_async_copy(sent, sent, send_r.at[k]).wait()
        sent = y.at[pl.ds(0, (m - 1) * sizes[k])]
        pltpu.make_async_copy(sent, sent, send_c.at[k]).wait()


def per_device(n, m, tracer, symbol_x, symbol_y, symbol_z):
    depth, ys, zs = tracer.shape
    height, length = ys * n, zs * m
    x_share, yc = depth // n, height // m
    sizes = piece_sizes(x_share)
    pieces = len(sizes)
    starts = [sum(sizes[:k]) for k in range(pieces)]
    block = min(height, 128)

    groups = [(0, 1)]
    while sum(groups[-1]) < pieces:
        first = sum(groups[-1])
        count = 1
        while first + count < pieces and n * sum(sizes[first : first + count + 1]) <= 128:
            count += 1
        groups.append((first, count))
    share = np.arange(depth).reshape(n, x_share)
    order = [share[:, a : a + e].reshape(-1) for a, e in zip(starts, sizes)]
    high, low = table_halves(depth)
    tab_x = []
    for first, count in groups:
        rows = np.concatenate(order[first : first + count])
        tab_x.append(left_table(high[rows], low[rows]))
    tab_x = np.concatenate(tab_x)
    high, low = table_halves(height)
    tab_y = [left_table(high[b : b + block], low[b : b + block]) for b in range(0, height, block)]
    tab_y = np.concatenate(tab_y)
    tab_zh, tab_zl = table_halves(length)

    anywhere = pl.BlockSpec(memory_space=pl.ANY)
    dma = pltpu.SemaphoreType.DMA
    regular = pltpu.SemaphoreType.REGULAR
    out = pl.pallas_call(
        functools.partial(kernel, n, m, sizes, groups, block),
        out_shape=pltpu.VMEM((x_share * yc, length), F32),
        in_specs=[anywhere] * 8,
        out_specs=pl.BlockSpec(memory_space=pltpu.VMEM),
        scratch_shapes=[
            pltpu.VMEM((depth, ys, zs), F32),
            pltpu.VMEM((depth, ys, zs), F32),
            pltpu.VMEM((x_share, height, zs), F32),
            pltpu.VMEM((m * x_share, yc, zs), F32),
            pltpu.VMEM((m * x_share, yc, zs), F32),
            pltpu.VMEM((x_share * yc, length), F32),
            pltpu.VMEM(tab_x.shape, BF16),
            pltpu.VMEM(tab_y.shape, BF16),
            pltpu.VMEM(tab_zh.shape, BF16),
            pltpu.VMEM(tab_zl.shape, BF16),
            pltpu.VMEM((depth, 128), F32),
            pltpu.VMEM((height, 128), F32),
            pltpu.VMEM((1, depth), F32),
            pltpu.VMEM((1, height), F32),
            pltpu.VMEM((1, length), F32),
            dma((8,)),
            dma((pieces,)),
            dma((pieces,)),
            dma((pieces,)),
            dma((pieces,)),
            regular((n // 2,)),
            regular,
        ],
        compiler_params=pltpu.CompilerParams(
            collective_id=0,
            has_side_effects=True,
            vmem_limit_bytes=(58 << 20) - 12 * x_share * yc * length,
        ),
    )(
        tracer,
        jnp.asarray(tab_x),
        jnp.asarray(tab_y),
        jnp.asarray(tab_zh),
        jnp.asarray(tab_zl),
        symbol_x[None],
        symbol_y[None],
        symbol_z[None],
    )
    return out.reshape(x_share, yc, length)


def solution(mesh):
    in_specs = (P(None, "row", "col"), P(), P(), P())
    out_specs = P("row", "col", None)
    body = functools.partial(per_device, mesh.shape["row"], mesh.shape["col"])
    return jax.shard_map(
        body, mesh=mesh, in_specs=in_specs, out_specs=out_specs, check_vma=False
    )
```

```python
import functools

import jax
import jax.numpy as jnp
import ml_dtypes
import numpy as np
from jax import lax
from jax.experimental import pallas as pl
from jax.experimental.pallas import tpu as pltpu
from jax.sharding import PartitionSpec as P

MESH = pl.DeviceIdType.MESH
F32 = jnp.float32
BF16 = jnp.bfloat16
PIECES = 8
LEAD = 1
OWN = 6
OWN_B = 3
BEGUN = 4
BEGUN_LOW = 5
LAG = 5
CUTS = 1


def table_halves(count):
    rank = np.arange(1, count + 1)
    turns = np.outer(rank, rank) % (2 * count + 2)
    table = np.sin(np.pi / (count + 1) * turns) * np.sqrt(2.0 / (count + 1))
    high = table.astype(ml_dtypes.bfloat16)
    low = (table - high.astype(np.float64)).astype(ml_dtypes.bfloat16)
    return high, low


def left_table(high, low):
    return np.concatenate(
        [np.concatenate([high, high], axis=1), np.concatenate([low, 0 * low], axis=1)]
    )


def halves(values):
    high = values.astype(BF16)
    return high, (values - high.astype(F32)).astype(BF16)


def dot(a, b):
    return jnp.dot(a, b, preferred_element_type=F32)


def from_left(table, values):
    rows = table.shape[0] // 2
    both = dot(table, jnp.concatenate(halves(values), axis=0))
    return both[:rows] + both[rows:]


def piece_sizes(share):
    size = max(1, share // PIECES)
    sizes = []
    left = share
    while left:
        size = min(size, left)
        if left <= size:
            size = max(1, left // 2)
        sizes.append(size)
        left -= size
    return sizes


def kernel(
    n, m, sizes, groups, block,
    field, tab_x, tab_y, tab_zh, tab_zl, sx, sy, sz, out,
    d, s, r, y, c, f, pass_on, tx, ty, tzh, tzl, colx, coly, vx, vy, vz,
    in_sem, send_r, recv_r, send_c, recv_c, recv_p, up_r, up_c,
):
    pieces = len(sizes)
    starts = [sum(sizes[:k]) for k in range(pieces)]
    lag, lead = min(LAG, pieces), min(LEAD, pieces - 1)
    me_r, me_c = lax.axis_index("row"), lax.axis_index("col")
    depth, ys, zs = d.shape
    yc = y.shape[1]
    cut = ys // CUTS
    fields = [pl.ds(i * cut, cut) for i in range(CUTS)]
    fields = [
        pltpu.make_async_copy(field.at[:, at, :], d.at[:, at, :], in_sem.at[8 + i])
        for i, at in enumerate(fields)
    ]
    loads = [(tab_x, tx, 1), (tab_y, ty, 2), (tab_zh, tzh, 3), (tab_zl, tzl, 4)]
    loads += [(sx, vx, 5), (sy, vy, 6), (sz, vz, 7)]
    loads = [pltpu.make_async_copy(a, b, in_sem.at[i]) for a, b, i in loads]

    odd = lax.rem(me_r, 2)
    tier = lax.div(me_r, 2)
    tiers = n // 2
    barrier = pltpu.get_barrier_semaphore()
    flip = 1 if m % 2 == 0 else 0
    place = lambda at: at ^ flip

    def greet_row(to, _):
        @pl.when(jnp.logical_or(odd == 0, lax.rem(to, 2) == 1))
        def _():
            pl.semaphore_signal(barrier, inc=1, device_id={"row": to}, device_id_type=MESH)

        return 0

    def greet_col(at, _):
        pl.semaphore_signal(barrier, inc=1, device_id={"col": place(at)}, device_id_type=MESH)
        return 0

    lax.fori_loop(me_r + 1, n, greet_row, 0)
    lax.fori_loop(place(me_c) + 1, m, greet_col, 0)
    for load in loads[:1] + fields + loads[1:]:
        load.start()
    earlier = jnp.where(odd == 1, me_r, tier) + place(me_c)

    @pl.when(earlier > 0)
    def _():
        pl.semaphore_wait(barrier, earlier)

    @pl.when(odd == 1)
    def _():
        def answer(to, _):
            pl.semaphore_signal(
                up_r.at[tier], inc=1, device_id={"row": to}, device_id_type=MESH
            )
            return 0

        lax.fori_loop(0, me_r, answer, 0)

    def answer_col(at, _):
        pl.semaphore_signal(up_c, inc=1, device_id={"col": place(at)}, device_id_type=MESH)
        return 0

    lax.fori_loop(0, place(me_c), answer_col, 0)

    loads[0].wait()
    lanes = d.reshape(depth * ys, zs)
    modes = s.reshape(s.shape[0] * ys, zs)

    def transform_x(first, count):
        begin = n * starts[first]
        rows = n * sum(sizes[first : first + count])
        table = tx[2 * begin : 2 * (begin + rows)]

        def pair(i, _):
            got = jnp.concatenate(
                [lanes[pl.ds(2 * i + h, depth, stride=ys), :] for h in range(2)], axis=1
            )
            got = from_left(table, got)
            for h in range(2):
                modes[pl.ds(begin * ys + 2 * i + h, rows, stride=ys), :] = got[
                    :, h * zs : (h + 1) * zs
                ]
            return 0

        for i in range(CUTS):
            if first == 0:
                fields[i].wait()
            lax.fori_loop(i * cut // 2, (i + 1) * cut // 2, pair, 0, unroll=True)

    def rows_of(at):
        return pl.ds(pl.multiple_of(at * ys, ys), ys)

    def send_row(k, to):
        each = sizes[k]
        pltpu.make_async_remote_copy(
            src_ref=s.at[pl.ds(n * starts[k] + to * each, each)],
            dst_ref=r.at[pl.ds(starts[k], each), rows_of(me_r), :],
            send_sem=send_r.at[k],
            recv_sem=recv_r.at[k],
            device_id={"row": to},
            device_id_type=MESH,
        ).start()

    def keep_row(k):
        each = sizes[k]
        r[pl.ds(starts[k], each), rows_of(me_r), :] = s[pl.ds(n * starts[k] + me_r * each, each)]

    def wait_up(at):
        pl.semaphore_wait(up_r.at[at], 1)

    half, step_out = tiers // 2, tiers // 4
    high = tier >= half
    low = jnp.logical_not(high)
    outer = jnp.logical_or(tier < step_out, tier >= tiers - step_out)
    inner = jnp.logical_not(outer)
    far, near = jnp.where(high, 0, half), jnp.where(high, half, 0)
    behind = jnp.where(high, me_r + 2 * step_out, me_r - 2 * step_out)
    ahead = jnp.where(high, me_r - 2 * step_out, me_r + 2 * step_out)
    every = range(pieces)

    def send_tier(k, at, other):
        send_row(k, 2 * at + (odd ^ other))

    def send_tiers(ks, begin, end, wait=False):
        def one(at, _):
            if wait:
                wait_up(at)
            for k in ks:
                for other in range(2):
                    send_row(k, 2 * at + other)
            return 0

        lax.fori_loop(begin, end, one, 0)

    def hand_on(k):
        each = sizes[k]
        pltpu.make_async_remote_copy(
            src_ref=s.at[pl.ds(n * starts[k] + 2 * far * each, n // 2 * each)],
            dst_ref=pass_on.at[pl.ds(n // 2 * starts[k], n // 2 * each)],
            send_sem=send_r.at[k],
            recv_sem=recv_p.at[k],
            device_id={"row": ahead},
            device_id_type=MESH,
        ).start()

    def got_pass(k):
        waited = pass_on.at[pl.ds(n // 2 * starts[k], n // 2 * sizes[k])]
        pltpu.make_async_copy(waited, waited, recv_p.at[k]).wait()

    def pass_rows(k, begin, end):
        each = sizes[k]

        def one(to, _):
            pltpu.make_async_remote_copy(
                src_ref=pass_on.at[pl.ds(n // 2 * starts[k] + (to - 2 * far) * each, each)],
                dst_ref=r.at[pl.ds(starts[k], each), rows_of(behind), :],
                send_sem=send_r.at[k],
                recv_sem=recv_r.at[k],
                device_id={"row": to},
                device_id_type=MESH,
            ).start()
            return 0

        lax.fori_loop(begin, end, one, 0)

    def own_rows(k, begin, end):
        def one(to, _):
            send_row(k, to)
            return 0

        lax.fori_loop(begin, end, one, 0)

    def hear_peer():
        @pl.when(odd == 0)
        def _():
            wait_up(tier)

    def start_far():
        for other in range(2):
            if other == 1:
                hear_peer()

            def one(at, _):
                send_tier(0, at, other)
                return 0

            lax.fori_loop(0, half, one, 0)

    def send_peer():
        for k in every:
            send_tier(k, tier, 1)

    begin, turn, end = 2 * far, jnp.where(high, 1, n), jnp.where(high, n // 2, n)

    def by_core(act):
        for core, own in enumerate((OWN, OWN_B)):

            @pl.when(lax.rem(me_c, 2) == core)
            def _():
                act(min(own, pieces))

    def cross(step, own):
        def part(step, begin, end):
            if 0 <= step < pieces:
                pass_rows(step, begin, end)
            for k in range(own, pieces):
                if k - max(1, 2 * own - 1 - k) == step:
                    own_rows(k, begin, end)

        if step < pieces:
            got_pass(step)
            part(step, begin, turn)
        if 0 <= step - lead:
            part(step - lead, turn, end)

    for at, (first, count) in enumerate(groups):
        transform_x(first, count)
        if at == 0:

            @pl.when(jnp.logical_and(high, inner))
            def _():
                start_far()

            @pl.when(jnp.logical_and(high, outer))
            def _():
                hand_on(0)

    begun_high, begun_low = min(BEGUN, pieces), min(BEGUN_LOW, pieces)

    @pl.when(jnp.logical_and(high, inner))
    def _():
        by_core(lambda own: [send_tiers([k], far, far + half) for k in range(1, own)])
        send_peer()
        send_tiers(every, tier + 1, tiers, wait=True)

    @pl.when(jnp.logical_and(low, inner))
    def _():
        hear_peer()
        send_tiers(every, 0, tier)
        send_peer()
        for at in range(half, tiers):
            wait_up(at)
            by_core(lambda own: send_tiers(range(own), at, at + 1))

    @pl.when(jnp.logical_and(high, outer))
    def _():
        hear_peer()
        for k in every:
            if k:
                hand_on(k)
            send_tiers([k], half, tier)
        send_peer()
        send_tiers(every, tier + 1, tiers, wait=True)

    @pl.when(jnp.logical_and(low, outer))
    def _():
        hear_peer()
        send_peer()
        send_tiers(every, 0, tier)

        def one(at, _):
            wait_up(at)
            return 0

        lax.fori_loop(tier + 1, half, one, 0)
        for k in every:
            hand_on(k)
            send_tiers([k], tier + 1, half)

    def crosses(steps):
        by_core(lambda own: [cross(step, own) for step in steps])

    def steps_from(step):
        return [at for at in range(step, pieces + lead) if at == step or step == pieces - 1] * (
            step < pieces
        )

    inner_high, inner_low = jnp.logical_and(high, inner), jnp.logical_and(low, inner)

    @pl.when(inner_high)
    def _():
        for step in range(begun_high):
            crosses(steps_from(step))

    @pl.when(inner_low)
    def _():
        for step in range(begun_low):
            crosses(steps_from(step))

    for k in every:
        keep_row(k)

    for load in loads[1:]:
        load.wait()

    def upright(row_ref, into):
        size = row_ref.shape[1]
        here = lax.broadcasted_iota(jnp.int32, (size, size), 0)
        there = lax.broadcasted_iota(jnp.int32, (size, size), 1)
        kept = jnp.where(here == there, row_ref[...], 0.0)
        into[...] = jnp.broadcast_to(jnp.sum(kept, axis=1, keepdims=True), into.shape)

    upright(vx, colx)
    upright(vy, coly)
    x_share = r.shape[0]
    part_y = coly[pl.ds(pl.multiple_of(me_c * yc, yc), yc), :]

    def factor(i, _):
        symbol = part_y + colx[pl.ds(me_r * x_share + i, 1), :]
        for at in range(0, vz.shape[1], 128):
            full = symbol + vz[:, at : at + 128]
            f[pl.ds(pl.multiple_of(i * yc, yc), yc), at : at + 128] = (1.0 - 0.2 * full) / (
                1.0 + 0.2 * full
            )
        return 0

    lax.fori_loop(0, x_share, factor, 0)

    @pl.when(place(me_c) < m - 1)
    def _():
        pl.semaphore_wait(up_c, m - 1 - place(me_c))

    def got_rows(k):
        waited = r.at[pl.ds(starts[k], sizes[k]), pl.ds(0, (n - 1) * ys), :]
        pltpu.make_async_copy(waited, waited, recv_r.at[k]).wait()

    def transform_y(k):
        each, base = sizes[k], m * starts[k]
        got = jnp.concatenate([r[starts[k] + j] for j in range(each)], axis=1)
        for b in range(ty.shape[0] // (2 * block)):
            now = from_left(ty[2 * b * block : 2 * (b + 1) * block], got)
            for q in range(block // yc):
                for j in range(each):
                    y[base + (b * (block // yc) + q) * each + j] = now[
                        q * yc : (q + 1) * yc, j * zs : (j + 1) * zs
                    ]

    def send_cols(k):
        each, base = sizes[k], m * starts[k]

        def one(i, _):
            to = lax.rem(me_c + i, m)
            pltpu.make_async_remote_copy(
                src_ref=y.at[pl.ds(base + to * each, each)],
                dst_ref=c.at[pl.ds(base + me_c * each, each)],
                send_sem=send_c.at[k],
                recv_sem=recv_c.at[k],
                device_id={"col": to},
                device_id_type=MESH,
            ).start()
            return 0

        lax.fori_loop(1, m, one, 0)
        own = pl.ds(base + me_c * each, each)
        c[own] = y[own]

    def got_cols(k):
        waited = c.at[pl.ds(m * starts[k], (m - 1) * sizes[k])]
        pltpu.make_async_copy(waited, waited, recv_c.at[k]).wait()

    def transform_z(k):
        each, base = sizes[k], m * starts[k]
        rows = each * yc
        got = jnp.concatenate(
            [c[base + q * each : base + (q + 1) * each].reshape(rows, zs) for q in range(m)],
            axis=1,
        )
        high, low = halves(got)
        both = dot(jnp.concatenate([high, low], axis=0), tzh[...])
        full = both[:rows] + both[rows:] + dot(high, tzl[...])
        at = slice(starts[k] * yc, starts[k] * yc + rows)
        out[at, :] = full * f[at, :]

    for k in range(pieces):
        got_rows(k)
        for which, begun in ((inner_high, begun_high), (inner_low, begun_low)):
            steps = steps_from(k + begun)
            if steps:

                @pl.when(which)
                def _():
                    crosses(steps)

        transform_y(k)
        send_cols(k)
        if k >= lag:
            got_cols(k - lag)
            transform_z(k - lag)
    def sent_rows(k):
        @pl.when(inner)
        def _():
            sent = pass_on.at[pl.ds(0, n // 2 * sizes[k])]
            pltpu.make_async_copy(sent, sent, send_r.at[k]).wait()

        sent = s.at[pl.ds(0, (n - 1) * sizes[k])]
        pltpu.make_async_copy(sent, sent, send_r.at[k]).wait()

    def sent_cols(k):
        sent = y.at[pl.ds(0, (m - 1) * sizes[k])]
        pltpu.make_async_copy(sent, sent, send_c.at[k]).wait()

    for k in range(pieces - lag, pieces):
        if k == pieces - 1:
            for j in every:
                sent_rows(j)
                sent_cols(j)

            @pl.when(jnp.logical_and(low, outer))
            def _():
                for at in range(half, tiers):
                    wait_up(at)

        got_cols(k)
        transform_z(k)


def per_device(n, m, tracer, symbol_x, symbol_y, symbol_z):
    depth, ys, zs = tracer.shape
    height, length = ys * n, zs * m
    x_share, yc = depth // n, height // m
    sizes = piece_sizes(x_share)
    pieces = len(sizes)
    starts = [sum(sizes[:k]) for k in range(pieces)]
    block = min(height, 128)

    groups = [(0, 1)]
    while sum(groups[-1]) < pieces:
        first = sum(groups[-1])
        count = 1
        while first + count < pieces and n * sum(sizes[first : first + count + 1]) <= 128:
            count += 1
        groups.append((first, count))
    share = np.arange(depth).reshape(n, x_share)
    order = [share[:, a : a + e].reshape(-1) for a, e in zip(starts, sizes)]
    high, low = table_halves(depth)
    tab_x = []
    for first, count in groups:
        rows = np.concatenate(order[first : first + count])
        tab_x.append(left_table(high[rows], low[rows]))
    tab_x = np.concatenate(tab_x)
    high, low = table_halves(height)
    tab_y = [left_table(high[b : b + block], low[b : b + block]) for b in range(0, height, block)]
    tab_y = np.concatenate(tab_y)
    tab_zh, tab_zl = table_halves(length)

    anywhere = pl.BlockSpec(memory_space=pl.ANY)
    dma = pltpu.SemaphoreType.DMA
    regular = pltpu.SemaphoreType.REGULAR
    out = pl.pallas_call(
        functools.partial(kernel, n, m, sizes, groups, block),
        out_shape=pltpu.VMEM((x_share * yc, length), F32),
        in_specs=[anywhere] * 8,
        out_specs=pl.BlockSpec(memory_space=pltpu.VMEM),
        scratch_shapes=[
            pltpu.VMEM((depth, ys, zs), F32),
            pltpu.VMEM((depth, ys, zs), F32),
            pltpu.VMEM((x_share, height, zs), F32),
            pltpu.VMEM((m * x_share, yc, zs), F32),
            pltpu.VMEM((m * x_share, yc, zs), F32),
            pltpu.VMEM((x_share * yc, length), F32),
            pltpu.VMEM((n // 2 * x_share, ys, zs), F32),
            pltpu.VMEM(tab_x.shape, BF16),
            pltpu.VMEM(tab_y.shape, BF16),
            pltpu.VMEM(tab_zh.shape, BF16),
            pltpu.VMEM(tab_zl.shape, BF16),
            pltpu.VMEM((depth, 128), F32),
            pltpu.VMEM((height, 128), F32),
            pltpu.VMEM((1, depth), F32),
            pltpu.VMEM((1, height), F32),
            pltpu.VMEM((1, length), F32),
            dma((8 + CUTS,)),
            dma((pieces,)),
            dma((pieces,)),
            dma((pieces,)),
            dma((pieces,)),
            dma((pieces,)),
            regular((n // 2,)),
            regular,
        ],
        compiler_params=pltpu.CompilerParams(
            collective_id=0,
            has_side_effects=True,
            vmem_limit_bytes=(58 << 20) - 12 * x_share * yc * length,
        ),
    )(
        tracer,
        jnp.asarray(tab_x),
        jnp.asarray(tab_y),
        jnp.asarray(tab_zh),
        jnp.asarray(tab_zl),
        symbol_x[None],
        symbol_y[None],
        symbol_z[None],
    )
    return out.reshape(x_share, yc, length)


def solution(mesh):
    in_specs = (P(None, "row", "col"), P(), P(), P())
    out_specs = P("row", "col", None)
    body = functools.partial(per_device, mesh.shape["row"], mesh.shape["col"])
    return jax.shard_map(
        body, mesh=mesh, in_specs=in_specs, out_specs=out_specs, check_vma=False
    )
```

```python
import functools

import jax
import jax.numpy as jnp
import ml_dtypes
import numpy as np
from jax import lax
from jax.experimental import pallas as pl
from jax.experimental.pallas import tpu as pltpu
from jax.sharding import PartitionSpec as P

MESH = pl.DeviceIdType.MESH
F32 = jnp.float32
BF16 = jnp.bfloat16
PIECES = 8
LEAD = 2
OWN = 6
OWN_B = 3
BEGUN = 5
BEGUN_LOW = 6
LAG = 5
CUTS = 1
NEAR_LAG = 5


def table_halves(count):
    rank = np.arange(1, count + 1)
    turns = np.outer(rank, rank) % (2 * count + 2)
    table = np.sin(np.pi / (count + 1) * turns) * np.sqrt(2.0 / (count + 1))
    high = table.astype(ml_dtypes.bfloat16)
    low = (table - high.astype(np.float64)).astype(ml_dtypes.bfloat16)
    return high, low


def left_table(high, low):
    return np.concatenate(
        [np.concatenate([high, high], axis=1), np.concatenate([low, 0 * low], axis=1)]
    )


def halves(values):
    high = values.astype(BF16)
    return high, (values - high.astype(F32)).astype(BF16)


def dot(a, b):
    return jnp.dot(a, b, preferred_element_type=F32)


def from_left(table, values):
    rows = table.shape[0] // 2
    both = dot(table, jnp.concatenate(halves(values), axis=0))
    return both[:rows] + both[rows:]


def piece_sizes(share):
    size = max(1, share // PIECES)
    sizes = []
    left = share
    while left:
        size = min(size, left)
        if left <= size:
            size = max(1, left // 2)
        sizes.append(size)
        left -= size
    return sizes


def kernel(
    n, m, sizes, groups, block,
    field, tab_x, tab_y, tab_zh, tab_zl, sx, sy, sz, out,
    d, s, r, y, c, f, pass_on, tx, ty, tzh, tzl, colx, coly, vx, vy, vz,
    in_sem, send_r, recv_r, send_c, recv_c, recv_p, up_r, up_c,
):
    pieces = len(sizes)
    starts = [sum(sizes[:k]) for k in range(pieces)]
    lag, lead = min(LAG, pieces), min(LEAD, pieces - 1)
    me_r, me_c = lax.axis_index("row"), lax.axis_index("col")
    depth, ys, zs = d.shape
    yc = y.shape[1]
    cut = ys // CUTS
    fields = [pl.ds(i * cut, cut) for i in range(CUTS)]
    fields = [
        pltpu.make_async_copy(field.at[:, at, :], d.at[:, at, :], in_sem.at[8 + i])
        for i, at in enumerate(fields)
    ]
    loads = [(tab_x, tx, 1), (tab_y, ty, 2), (tab_zh, tzh, 3), (tab_zl, tzl, 4)]
    loads += [(sx, vx, 5), (sy, vy, 6), (sz, vz, 7)]
    loads = [pltpu.make_async_copy(a, b, in_sem.at[i]) for a, b, i in loads]

    odd = lax.rem(me_r, 2)
    tier = lax.div(me_r, 2)
    tiers = n // 2
    barrier = pltpu.get_barrier_semaphore()
    flip = 1 if m % 2 == 0 else 0
    place = lambda at: at ^ flip

    def greet_row(to, _):
        @pl.when(jnp.logical_or(odd == 0, lax.rem(to, 2) == 1))
        def _():
            pl.semaphore_signal(barrier, inc=1, device_id={"row": to}, device_id_type=MESH)

        return 0

    def greet_col(at, _):
        pl.semaphore_signal(barrier, inc=1, device_id={"col": place(at)}, device_id_type=MESH)
        return 0

    lax.fori_loop(me_r + 1, n, greet_row, 0)
    lax.fori_loop(place(me_c) + 1, m, greet_col, 0)
    for load in loads[:1] + fields + loads[1:]:
        load.start()
    earlier = jnp.where(odd == 1, me_r, tier) + place(me_c)

    @pl.when(earlier > 0)
    def _():
        pl.semaphore_wait(barrier, earlier)

    @pl.when(odd == 1)
    def _():
        def answer(to, _):
            pl.semaphore_signal(
                up_r.at[tier], inc=1, device_id={"row": to}, device_id_type=MESH
            )
            return 0

        lax.fori_loop(0, me_r, answer, 0)

    def answer_col(at, _):
        pl.semaphore_signal(up_c, inc=1, device_id={"col": place(at)}, device_id_type=MESH)
        return 0

    lax.fori_loop(0, place(me_c), answer_col, 0)

    loads[0].wait()
    lanes = d.reshape(depth * ys, zs)
    modes = s.reshape(s.shape[0] * ys, zs)

    def transform_x(first, count):
        begin = n * starts[first]
        rows = n * sum(sizes[first : first + count])
        table = tx[2 * begin : 2 * (begin + rows)]

        def pair(i, _):
            got = jnp.concatenate(
                [lanes[pl.ds(2 * i + h, depth, stride=ys), :] for h in range(2)], axis=1
            )
            got = from_left(table, got)
            for h in range(2):
                modes[pl.ds(begin * ys + 2 * i + h, rows, stride=ys), :] = got[
                    :, h * zs : (h + 1) * zs
                ]
            return 0

        for i in range(CUTS):
            if first == 0:
                fields[i].wait()
            lax.fori_loop(i * cut // 2, (i + 1) * cut // 2, pair, 0, unroll=True)

    def rows_of(at):
        return pl.ds(pl.multiple_of(at * ys, ys), ys)

    def send_row(k, to):
        each = sizes[k]
        pltpu.make_async_remote_copy(
            src_ref=s.at[pl.ds(n * starts[k] + to * each, each)],
            dst_ref=r.at[pl.ds(starts[k], each), rows_of(me_r), :],
            send_sem=send_r,
            recv_sem=recv_r.at[k],
            device_id={"row": to},
            device_id_type=MESH,
        ).start()

    def keep_row(k):
        each = sizes[k]
        r[pl.ds(starts[k], each), rows_of(me_r), :] = s[pl.ds(n * starts[k] + me_r * each, each)]

    def wait_up(at):
        pl.semaphore_wait(up_r.at[at], 1)

    half, step_out = tiers // 2, tiers // 4
    high = tier >= half
    low = jnp.logical_not(high)
    outer = jnp.logical_or(tier < step_out, tier >= tiers - step_out)
    inner = jnp.logical_not(outer)
    far, near = jnp.where(high, 0, half), jnp.where(high, half, 0)
    behind = jnp.where(high, me_r + 2 * step_out, me_r - 2 * step_out)
    ahead = jnp.where(high, me_r - 2 * step_out, me_r + 2 * step_out)
    every, near_lag = range(pieces), min(NEAR_LAG, pieces)

    def send_tier(k, at, other):
        send_row(k, 2 * at + (odd ^ other))

    def send_tiers(ks, begin, end, wait=False):
        def one(at, _):
            if wait:
                wait_up(at)
            for k in ks:
                for other in range(2):
                    send_row(k, 2 * at + other)
            return 0

        lax.fori_loop(begin, end, one, 0)

    def hand_on(k):
        each = sizes[k]
        pltpu.make_async_remote_copy(
            src_ref=s.at[pl.ds(n * starts[k] + 2 * far * each, n // 2 * each)],
            dst_ref=pass_on.at[pl.ds(n // 2 * starts[k], n // 2 * each)],
            send_sem=send_r,
            recv_sem=recv_p.at[k],
            device_id={"row": ahead},
            device_id_type=MESH,
        ).start()

    def got_pass(k):
        waited = pass_on.at[pl.ds(n // 2 * starts[k], n // 2 * sizes[k])]
        pltpu.make_async_copy(waited, waited, recv_p.at[k]).wait()

    def pass_rows(k, begin, end):
        each = sizes[k]

        def one(to, _):
            pltpu.make_async_remote_copy(
                src_ref=pass_on.at[pl.ds(n // 2 * starts[k] + (to - 2 * far) * each, each)],
                dst_ref=r.at[pl.ds(starts[k], each), rows_of(behind), :],
                send_sem=send_r,
                recv_sem=recv_r.at[k],
                device_id={"row": to},
                device_id_type=MESH,
            ).start()
            return 0

        lax.fori_loop(begin, end, one, 0)

    def own_rows(k, begin, end):
        def one(to, _):
            send_row(k, to)
            return 0

        lax.fori_loop(begin, end, one, 0)

    def hear_peer():
        @pl.when(odd == 0)
        def _():
            wait_up(tier)

    def start_far():
        for other in range(2):
            if other == 1:
                hear_peer()

            def one(at, _):
                send_tier(0, at, other)
                return 0

            lax.fori_loop(0, half, one, 0)

    def send_peer():
        for k in every:
            send_tier(k, tier, 1)

    begin, turn, end = 2 * far, jnp.where(high, 1, n), jnp.where(high, n // 2, n)

    def by_core(act):
        for core, own in enumerate((OWN, OWN_B)):

            @pl.when(lax.rem(me_c, 2) == core)
            def _():
                act(min(own, pieces))

    def cross(step, own):
        def part(step, begin, end):
            if 0 <= step < pieces:
                pass_rows(step, begin, end)
            for k in range(own, pieces):
                if k - max(1, 2 * own - 1 - k) == step:
                    own_rows(k, begin, end)

        if step < pieces:
            got_pass(step)
            part(step, begin, turn)
        if 0 <= step - lead:
            part(step - lead, turn, end)

    for at, (first, count) in enumerate(groups):
        transform_x(first, count)
        if at == 0:

            @pl.when(jnp.logical_and(high, inner))
            def _():
                start_far()

            @pl.when(jnp.logical_and(high, outer))
            def _():
                hand_on(0)

    begun_high, begun_low = min(BEGUN, pieces), min(BEGUN_LOW, pieces)

    @pl.when(jnp.logical_and(high, inner))
    def _():
        by_core(lambda own: [send_tiers([k], far, far + half) for k in range(1, own)])
        send_peer()
        send_tiers(every, tier + 1, tiers, wait=True)

    @pl.when(jnp.logical_and(low, inner))
    def _():
        hear_peer()
        send_tiers(every, 0, tier)
        send_peer()
        for at in range(half, tiers):
            wait_up(at)
            by_core(lambda own: send_tiers(range(own), at, at + 1))

    @pl.when(jnp.logical_and(high, outer))
    def _():
        hear_peer()
        for k in range(pieces + near_lag):
            if 0 < k < pieces:
                hand_on(k)
            if k >= near_lag:
                send_tiers([k - near_lag], half, tier)
        send_peer()
        send_tiers(every, tier + 1, tiers, wait=True)

    @pl.when(jnp.logical_and(low, outer))
    def _():
        hear_peer()
        send_peer()
        send_tiers(every, 0, tier)

        def one(at, _):
            wait_up(at)
            return 0

        lax.fori_loop(tier + 1, half, one, 0)
        for k in range(pieces + near_lag):
            if k < pieces:
                hand_on(k)
            if k >= near_lag:
                send_tiers([k - near_lag], tier + 1, half)

    def crosses(steps):
        by_core(lambda own: [cross(step, own) for step in steps])

    def steps_from(step):
        return [at for at in range(step, pieces + lead) if at == step or step == pieces - 1] * (
            step < pieces
        )

    inner_high, inner_low = jnp.logical_and(high, inner), jnp.logical_and(low, inner)

    @pl.when(inner_high)
    def _():
        for step in range(begun_high):
            crosses(steps_from(step))

    @pl.when(inner_low)
    def _():
        for step in range(begun_low):
            crosses(steps_from(step))

    for k in every:
        keep_row(k)

    for load in loads[1:]:
        load.wait()

    def upright(row_ref, into):
        size = row_ref.shape[1]
        here = lax.broadcasted_iota(jnp.int32, (size, size), 0)
        there = lax.broadcasted_iota(jnp.int32, (size, size), 1)
        kept = jnp.where(here == there, row_ref[...], 0.0)
        into[...] = jnp.broadcast_to(jnp.sum(kept, axis=1, keepdims=True), into.shape)

    upright(vx, colx)
    upright(vy, coly)
    x_share = r.shape[0]
    part_y = coly[pl.ds(pl.multiple_of(me_c * yc, yc), yc), :]

    def factor(i, _):
        symbol = part_y + colx[pl.ds(me_r * x_share + i, 1), :]
        for at in range(0, vz.shape[1], 128):
            full = symbol + vz[:, at : at + 128]
            f[pl.ds(pl.multiple_of(i * yc, yc), yc), at : at + 128] = (1.0 - 0.2 * full) / (
                1.0 + 0.2 * full
            )
        return 0

    lax.fori_loop(0, x_share, factor, 0)

    @pl.when(place(me_c) < m - 1)
    def _():
        pl.semaphore_wait(up_c, m - 1 - place(me_c))

    def got_rows(k):
        waited = r.at[pl.ds(starts[k], sizes[k]), pl.ds(0, (n - 1) * ys), :]
        pltpu.make_async_copy(waited, waited, recv_r.at[k]).wait()

    def transform_y(k):
        each, base = sizes[k], m * starts[k]
        got = jnp.concatenate([r[starts[k] + j] for j in range(each)], axis=1)
        for b in range(ty.shape[0] // (2 * block)):
            now = from_left(ty[2 * b * block : 2 * (b + 1) * block], got)
            for q in range(block // yc):
                for j in range(each):
                    y[base + (b * (block // yc) + q) * each + j] = now[
                        q * yc : (q + 1) * yc, j * zs : (j + 1) * zs
                    ]

    def send_cols(k):
        each, base = sizes[k], m * starts[k]

        def one(i, _):
            to = lax.rem(me_c + i, m)
            pltpu.make_async_remote_copy(
                src_ref=y.at[pl.ds(base + to * each, each)],
                dst_ref=c.at[pl.ds(base + me_c * each, each)],
                send_sem=send_c,
                recv_sem=recv_c.at[k],
                device_id={"col": to},
                device_id_type=MESH,
            ).start()
            return 0

        lax.fori_loop(1, m, one, 0)
        own = pl.ds(base + me_c * each, each)
        c[own] = y[own]

    def got_cols(k):
        waited = c.at[pl.ds(m * starts[k], (m - 1) * sizes[k])]
        pltpu.make_async_copy(waited, waited, recv_c.at[k]).wait()

    def transform_z(k):
        each, base = sizes[k], m * starts[k]
        rows = each * yc
        got = jnp.concatenate(
            [c[base + q * each : base + (q + 1) * each].reshape(rows, zs) for q in range(m)],
            axis=1,
        )
        high, low = halves(got)
        both = dot(jnp.concatenate([high, low], axis=0), tzh[...])
        full = both[:rows] + both[rows:] + dot(high, tzl[...])
        at = slice(starts[k] * yc, starts[k] * yc + rows)
        out[at, :] = full * f[at, :]

    for k in range(pieces):
        got_rows(k)
        for which, begun in ((inner_high, begun_high), (inner_low, begun_low)):
            steps = steps_from(k + begun)
            if steps:

                @pl.when(which)
                def _():
                    crosses(steps)

        transform_y(k)
        send_cols(k)
        if k >= lag:
            got_cols(k - lag)
            transform_z(k - lag)
    def sent_all():
        @pl.when(inner)
        def _():
            pltpu.make_async_copy(pass_on, pass_on, send_r).wait()

        sent = s.at[pl.ds(0, (n - 1) * x_share)]
        pltpu.make_async_copy(sent, sent, send_r).wait()

    def sent_cols():
        sent = y.at[pl.ds(0, (m - 1) * x_share)]
        pltpu.make_async_copy(sent, sent, send_c).wait()

    for k in range(pieces - lag, pieces):
        if k == pieces - 1:
            sent_all()

            @pl.when(jnp.logical_and(low, outer))
            def _():
                for at in range(half, tiers):
                    wait_up(at)

        got_cols(k)
        transform_z(k)
    sent_cols()


def per_device(n, m, tracer, symbol_x, symbol_y, symbol_z):
    depth, ys, zs = tracer.shape
    height, length = ys * n, zs * m
    x_share, yc = depth // n, height // m
    sizes = piece_sizes(x_share)
    pieces = len(sizes)
    starts = [sum(sizes[:k]) for k in range(pieces)]
    block = min(height, 128)

    groups = [(0, 1)]
    while sum(groups[-1]) < pieces:
        first = sum(groups[-1])
        count = 1
        while first + count < pieces and n * sum(sizes[first : first + count + 1]) <= 128:
            count += 1
        groups.append((first, count))
    share = np.arange(depth).reshape(n, x_share)
    order = [share[:, a : a + e].reshape(-1) for a, e in zip(starts, sizes)]
    high, low = table_halves(depth)
    tab_x = []
    for first, count in groups:
        rows = np.concatenate(order[first : first + count])
        tab_x.append(left_table(high[rows], low[rows]))
    tab_x = np.concatenate(tab_x)
    high, low = table_halves(height)
    tab_y = [left_table(high[b : b + block], low[b : b + block]) for b in range(0, height, block)]
    tab_y = np.concatenate(tab_y)
    tab_zh, tab_zl = table_halves(length)

    anywhere = pl.BlockSpec(memory_space=pl.ANY)
    dma = pltpu.SemaphoreType.DMA
    regular = pltpu.SemaphoreType.REGULAR
    out = pl.pallas_call(
        functools.partial(kernel, n, m, sizes, groups, block),
        out_shape=pltpu.VMEM((x_share * yc, length), F32),
        in_specs=[anywhere] * 8,
        out_specs=pl.BlockSpec(memory_space=pltpu.VMEM),
        scratch_shapes=[
            pltpu.VMEM((depth, ys, zs), F32),
            pltpu.VMEM((depth, ys, zs), F32),
            pltpu.VMEM((x_share, height, zs), F32),
            pltpu.VMEM((m * x_share, yc, zs), F32),
            pltpu.VMEM((m * x_share, yc, zs), F32),
            pltpu.VMEM((x_share * yc, length), F32),
            pltpu.VMEM((n // 2 * x_share, ys, zs), F32),
            pltpu.VMEM(tab_x.shape, BF16),
            pltpu.VMEM(tab_y.shape, BF16),
            pltpu.VMEM(tab_zh.shape, BF16),
            pltpu.VMEM(tab_zl.shape, BF16),
            pltpu.VMEM((depth, 128), F32),
            pltpu.VMEM((height, 128), F32),
            pltpu.VMEM((1, depth), F32),
            pltpu.VMEM((1, height), F32),
            pltpu.VMEM((1, length), F32),
            dma((8 + CUTS,)),
            dma,
            dma((pieces,)),
            dma,
            dma((pieces,)),
            dma((pieces,)),
            regular((n // 2,)),
            regular,
        ],
        compiler_params=pltpu.CompilerParams(
            collective_id=0,
            has_side_effects=True,
            vmem_limit_bytes=(58 << 20) - 12 * x_share * yc * length,
        ),
    )(
        tracer,
        jnp.asarray(tab_x),
        jnp.asarray(tab_y),
        jnp.asarray(tab_zh),
        jnp.asarray(tab_zl),
        symbol_x[None],
        symbol_y[None],
        symbol_z[None],
    )
    return out.reshape(x_share, yc, length)


def solution(mesh):
    in_specs = (P(None, "row", "col"), P(), P(), P())
    out_specs = P("row", "col", None)
    body = functools.partial(per_device, mesh.shape["row"], mesh.shape["col"])
    return jax.shard_map(
        body, mesh=mesh, in_specs=in_specs, out_specs=out_specs, check_vma=False
    )
```

```python
import functools

import jax
import jax.numpy as jnp
import ml_dtypes
import numpy as np
from jax import lax
from jax.experimental import pallas as pl
from jax.experimental.pallas import tpu as pltpu
from jax.sharding import PartitionSpec as P

MESH = pl.DeviceIdType.MESH
F32 = jnp.float32
BF16 = jnp.bfloat16
PIECES = 8
LEAD = 2
OWN = 6
OWN_B = 3
BEGUN = 6
BEGUN_LOW = 6
LAG = 6
CUTS = 2
NEAR_LAG = 5


def table_halves(count):
    rank = np.arange(1, count + 1)
    turns = np.outer(rank, rank) % (2 * count + 2)
    table = np.sin(np.pi / (count + 1) * turns) * np.sqrt(2.0 / (count + 1))
    high = table.astype(ml_dtypes.bfloat16)
    low = (table - high.astype(np.float64)).astype(ml_dtypes.bfloat16)
    return high, low


def left_table(high, low):
    return np.concatenate(
        [np.concatenate([high, high], axis=1), np.concatenate([low, 0 * low], axis=1)]
    )


def halves(values):
    high = values.astype(BF16)
    return high, (values - high.astype(F32)).astype(BF16)


def dot(a, b):
    return jnp.dot(a, b, preferred_element_type=F32)


def from_left(table, values):
    rows = table.shape[0] // 2
    both = dot(table, jnp.concatenate(halves(values), axis=0))
    return both[:rows] + both[rows:]


def piece_sizes(share):
    size = max(1, share // PIECES)
    sizes = []
    left = share
    while left:
        now = size if 4 * left > share else max(1, size // 2)
        sizes.append(min(now, left))
        left -= sizes[-1]
    return sizes


def kernel(
    n, m, sizes, groups, block,
    field, tab_x, tab_y, tab_zh, tab_zl, sx, sy, sz, out,
    d, s, r, y, c, f, pass_on, tx, ty, tzh, tzl, colx, coly, vx, vy, vz,
    in_sem, send_r, recv_r, send_c, recv_c, recv_p, up_r, up_c, up_e,
):
    pieces = len(sizes)
    starts = [sum(sizes[:k]) for k in range(pieces)]
    lag, lead = min(LAG, pieces), min(LEAD, pieces - 1)
    me_r, me_c = lax.axis_index("row"), lax.axis_index("col")
    depth, ys, zs = d.shape
    yc = y.shape[1]
    cut = ys // CUTS
    fields = [pl.ds(i * cut, cut) for i in range(CUTS)]
    fields = [
        pltpu.make_async_copy(field.at[:, at, :], d.at[:, at, :], in_sem.at[2 + i])
        for i, at in enumerate(fields)
    ]
    loads = [(tab_x, tx, 0), (tab_y, ty, 1), (tab_zh, tzh, 1), (tab_zl, tzl, 1)]
    loads += [(sx, vx, 1), (sy, vy, 1), (sz, vz, 1)]
    loads = [pltpu.make_async_copy(a, b, in_sem.at[i]) for a, b, i in loads]

    for load in fields + loads:
        load.start()

    odd = lax.rem(me_r, 2)
    tier = lax.div(me_r, 2)
    tiers = n // 2
    barrier = pltpu.get_barrier_semaphore()
    flip = 1 if m % 2 == 0 else 0
    place = lambda at: at ^ flip

    def greet_row(to, _):
        @pl.when(jnp.logical_or(odd == 0, lax.rem(to, 2) == 1))
        def _():
            pl.semaphore_signal(barrier, inc=1, device_id={"row": to}, device_id_type=MESH)

        return 0

    def greet_col(at, _):
        pl.semaphore_signal(barrier, inc=1, device_id={"col": place(at)}, device_id_type=MESH)
        return 0

    lax.fori_loop(me_r + 1, n, greet_row, 0)
    lax.fori_loop(place(me_c) + 1, m, greet_col, 0)
    earlier = jnp.where(odd == 1, me_r, tier) + place(me_c)

    @pl.when(earlier > 0)
    def _():
        pl.semaphore_wait(barrier, earlier)

    @pl.when(odd == 1)
    def _():
        def answer(to, _):
            pl.semaphore_signal(
                up_r.at[tier], inc=1, device_id={"row": to}, device_id_type=MESH
            )
            return 0

        lax.fori_loop(0, me_r, answer, 0)

    @pl.when(me_r == 2 * (tiers // 2))
    def _():
        for at in range(tiers // 4, tiers // 2):
            pl.semaphore_signal(up_e, inc=1, device_id={"row": 2 * at}, device_id_type=MESH)

    def answer_col(at, _):
        pl.semaphore_signal(up_c, inc=1, device_id={"col": place(at)}, device_id_type=MESH)
        return 0

    lax.fori_loop(0, place(me_c), answer_col, 0)

    loads[0].wait()
    lanes = d.reshape(depth * ys, zs)
    modes = s.reshape(s.shape[0] * ys, zs)

    def transform_x(first, count, after=None):
        begin = n * starts[first]
        rows = n * sum(sizes[first : first + count])
        table = tx[2 * begin : 2 * (begin + rows)]

        def pair(i, _):
            got = jnp.concatenate(
                [lanes[pl.ds(2 * i + h, depth, stride=ys), :] for h in range(2)], axis=1
            )
            got = from_left(table, got)
            for h in range(2):
                modes[pl.ds(begin * ys + 2 * i + h, rows, stride=ys), :] = got[
                    :, h * zs : (h + 1) * zs
                ]
            return 0

        for i in range(CUTS):
            if first == 0:
                fields[i].wait()
            lax.fori_loop(i * cut // 2, (i + 1) * cut // 2, pair, 0, unroll=True)
            if after is not None:
                after(i)

    def rows_of(at):
        return pl.ds(pl.multiple_of(at * ys, ys), ys)

    def send_row(k, to, part=0, parts=1):
        each, some = sizes[k], ys // parts
        into = pl.ds(pl.multiple_of(me_r * ys + part * some, some), some)
        pltpu.make_async_remote_copy(
            src_ref=s.at[pl.ds(n * starts[k] + to * each, each), pl.ds(part * some, some), :],
            dst_ref=r.at[pl.ds(starts[k], each), into, :],
            send_sem=send_r,
            recv_sem=recv_r.at[k],
            device_id={"row": to},
            device_id_type=MESH,
        ).start()

    def keep_row(k):
        each = sizes[k]
        r[pl.ds(starts[k], each), rows_of(me_r), :] = s[pl.ds(n * starts[k] + me_r * each, each)]

    def wait_up(at):
        pl.semaphore_wait(up_r.at[at], 1)

    half, step_out = tiers // 2, tiers // 4
    high = tier >= half
    low = jnp.logical_not(high)
    outer = jnp.logical_or(tier < step_out, tier >= tiers - step_out)
    inner = jnp.logical_not(outer)
    far, near = jnp.where(high, 0, half), jnp.where(high, half, 0)
    behind = jnp.where(high, me_r + 2 * step_out, me_r - 2 * step_out)
    ahead = jnp.where(high, me_r - 2 * step_out, me_r + 2 * step_out)
    every, near_lag = range(pieces), min(NEAR_LAG, pieces)

    def send_tier(k, at, other):
        send_row(k, 2 * at + (odd ^ other))

    def send_tiers(ks, begin, end, wait=False):
        def one(at, _):
            if wait:
                wait_up(at)
            for k in ks:
                for other in range(2):
                    send_row(k, 2 * at + other)
            return 0

        lax.fori_loop(begin, end, one, 0)

    def hand_on(k):
        each = sizes[k]
        pltpu.make_async_remote_copy(
            src_ref=s.at[pl.ds(n * starts[k] + 2 * far * each, n // 2 * each)],
            dst_ref=pass_on.at[pl.ds(n // 2 * starts[k], n // 2 * each)],
            send_sem=send_r,
            recv_sem=recv_p.at[k],
            device_id={"row": ahead},
            device_id_type=MESH,
        ).start()

    def got_pass(k):
        waited = pass_on.at[pl.ds(n // 2 * starts[k], n // 2 * sizes[k])]
        pltpu.make_async_copy(waited, waited, recv_p.at[k]).wait()

    def pass_rows(k, begin, end):
        each = sizes[k]

        def one(to, _):
            pltpu.make_async_remote_copy(
                src_ref=pass_on.at[pl.ds(n // 2 * starts[k] + (to - 2 * far) * each, each)],
                dst_ref=r.at[pl.ds(starts[k], each), rows_of(behind), :],
                send_sem=send_r,
                recv_sem=recv_r.at[k],
                device_id={"row": to},
                device_id_type=MESH,
            ).start()
            return 0

        lax.fori_loop(begin, end, one, 0)

    def own_rows(k, begin, end):
        def one(to, _):
            send_row(k, to)
            return 0

        lax.fori_loop(begin, end, one, 0)

    def hear_peer():
        @pl.when(odd == 0)
        def _():
            wait_up(tier)

    def start_far(part):
        def same(at, _):
            send_row(0, 2 * at + odd, part, CUTS)
            return 0

        lax.fori_loop(0, half, same, 0)

        if part == CUTS - 1:
            hear_peer()

            def other(at, _):
                send_tier(0, at, 1)
                return 0

            lax.fori_loop(0, half, other, 0)

    def start_low():
        @pl.when(odd == 0)
        def _():
            pl.semaphore_wait(up_e, 1)
            send_tier(0, half, 0)

        @pl.when(odd == 1)
        def _():
            wait_up(half)
            send_tier(0, half, 0)
            send_tier(0, half, 1)

    def send_peer():
        for k in every:
            send_tier(k, tier, 1)

    begin, turn, end = 2 * far, jnp.where(high, 1, n), jnp.where(high, n // 2, n)

    def by_core(act):
        for core, own in enumerate((OWN, OWN_B)):

            @pl.when(lax.rem(me_c, 2) == core)
            def _():
                act(min(own, pieces))

    def cross(step, own):
        def part(step, begin, end):
            if 0 <= step < pieces:
                pass_rows(step, begin, end)
            for k in range(own, pieces):
                if k - max(1, 2 * own - 1 - k) == step:
                    own_rows(k, begin, end)

        if step < pieces:
            got_pass(step)
            part(step, begin, turn)
        if 0 <= step - lead:
            part(step - lead, turn, end)

    inner_high, inner_low = jnp.logical_and(high, inner), jnp.logical_and(low, inner)
    begun_high, begun_low = min(BEGUN, pieces), min(BEGUN_LOW, pieces)

    def first_sends(part):
        @pl.when(inner_high)
        def _():
            start_far(part)

        if part == CUTS - 1:

            @pl.when(inner_low)
            def _():
                start_low()

            @pl.when(jnp.logical_and(high, outer))
            def _():
                hand_on(0)

    for at, (first, count) in enumerate(groups):
        transform_x(first, count, None if at else first_sends)

    @pl.when(jnp.logical_and(high, inner))
    def _():
        by_core(lambda own: [send_tiers([k], far, far + half) for k in range(1, own)])
        send_peer()
        send_tiers(every, tier + 1, tiers, wait=True)

    @pl.when(inner_low)
    def _():
        def more(own):
            for k in range(1, own):
                send_tier(k, half, 0)

        by_core(more)
        hear_peer()
        send_tiers(every, 0, tier)
        send_peer()

        @pl.when(odd == 0)
        def _():
            wait_up(half)
            send_tier(0, half, 1)

        def others(own):
            for k in range(1, own):
                send_tier(k, half, 1)

        by_core(others)
        for at in range(half + 1, tiers):
            wait_up(at)
            by_core(lambda own: send_tiers(range(own), at, at + 1))

    @pl.when(jnp.logical_and(high, outer))
    def _():
        hear_peer()
        for k in range(pieces + near_lag):
            if 0 < k < pieces:
                hand_on(k)
            if k >= near_lag:
                send_tiers([k - near_lag], half, tier)
        send_peer()
        send_tiers(every, tier + 1, tiers, wait=True)

    @pl.when(jnp.logical_and(low, outer))
    def _():
        hear_peer()
        send_peer()
        send_tiers(every, 0, tier)

        def one(at, _):
            wait_up(at)
            return 0

        lax.fori_loop(tier + 1, half, one, 0)
        for k in range(pieces + near_lag):
            if k < pieces:
                hand_on(k)
            if k >= near_lag:
                send_tiers([k - near_lag], tier + 1, half)

    def crosses(steps):
        by_core(lambda own: [cross(step, own) for step in steps])

    def steps_from(step):
        return [at for at in range(step, pieces + lead) if at == step or step == pieces - 1] * (
            step < pieces
        )

    @pl.when(inner_high)
    def _():
        for step in range(begun_high):
            crosses(steps_from(step))

    @pl.when(inner_low)
    def _():
        for step in range(begun_low):
            crosses(steps_from(step))

    for k in every:
        keep_row(k)

    for load in loads[1:]:
        load.wait()

    def upright(row_ref, into):
        size = row_ref.shape[1]
        here = lax.broadcasted_iota(jnp.int32, (size, size), 0)
        there = lax.broadcasted_iota(jnp.int32, (size, size), 1)
        kept = jnp.where(here == there, row_ref[...], 0.0)
        into[...] = jnp.broadcast_to(jnp.sum(kept, axis=1, keepdims=True), into.shape)

    upright(vx, colx)
    upright(vy, coly)
    x_share = r.shape[0]
    part_y = coly[pl.ds(pl.multiple_of(me_c * yc, yc), yc), :]

    def factor(i, _):
        symbol = part_y + colx[pl.ds(me_r * x_share + i, 1), :]
        for at in range(0, vz.shape[1], 128):
            full = symbol + vz[:, at : at + 128]
            f[pl.ds(pl.multiple_of(i * yc, yc), yc), at : at + 128] = (1.0 - 0.2 * full) / (
                1.0 + 0.2 * full
            )
        return 0

    lax.fori_loop(0, x_share, factor, 0)

    @pl.when(place(me_c) < m - 1)
    def _():
        pl.semaphore_wait(up_c, m - 1 - place(me_c))

    def got_rows(k):
        waited = r.at[pl.ds(starts[k], sizes[k]), pl.ds(0, (n - 1) * ys), :]
        pltpu.make_async_copy(waited, waited, recv_r.at[k]).wait()

    def transform_y(k):
        each, base = sizes[k], m * starts[k]
        got = jnp.concatenate([r[starts[k] + j] for j in range(each)], axis=1)
        for b in range(ty.shape[0] // (2 * block)):
            now = from_left(ty[2 * b * block : 2 * (b + 1) * block], got)
            for q in range(block // yc):
                for j in range(each):
                    y[base + (b * (block // yc) + q) * each + j] = now[
                        q * yc : (q + 1) * yc, j * zs : (j + 1) * zs
                    ]

    def send_cols(k):
        each, base = sizes[k], m * starts[k]

        def one(i, _):
            to = lax.rem(me_c + i, m)
            beside = (lax.div(to, m // 2) == side).astype(jnp.int32) if k == pieces - 1 else 0
            pltpu.make_async_remote_copy(
                src_ref=y.at[pl.ds(base + to * each, each)],
                dst_ref=c.at[pl.ds(base + me_c * each, each)],
                send_sem=send_c,
                recv_sem=recv_c.at[k + beside],
                device_id={"col": to},
                device_id_type=MESH,
            ).start()
            return 0

        lax.fori_loop(1, m, one, 0)
        own = pl.ds(base + me_c * each, each)
        c[own] = y[own]

    def got_cols(k):
        waited = c.at[pl.ds(m * starts[k], (m - 1) * sizes[k])]
        pltpu.make_async_copy(waited, waited, recv_c.at[k]).wait()

    side = lax.div(me_c, m // 2)

    def half_z(at_side, count, sem):
        k = pieces - 1
        each, base = sizes[k], m * starts[k]
        rows, many = each * yc, m // 2 * zs
        if count:
            waited = c.at[pl.ds(base, count * each)]
            pltpu.make_async_copy(waited, waited, recv_c.at[sem]).wait()
        got = [
            c[pl.ds(base + (at_side * (m // 2) + q) * each, each)].reshape(rows, zs)
            for q in range(m // 2)
        ]
        high, low = halves(jnp.concatenate(got, axis=1))
        some = pl.ds(pl.multiple_of(at_side * many, many), many)
        both = dot(jnp.concatenate([high, low], axis=0), tzh[some, :])
        return both[:rows] + both[rows:] + dot(high, tzl[some, :])

    last_rows = slice(starts[pieces - 1] * yc, (starts[pieces - 1] + sizes[pieces - 1]) * yc)

    def transform_z(k):
        each, base = sizes[k], m * starts[k]
        rows = each * yc
        got = jnp.concatenate(
            [c[base + q * each : base + (q + 1) * each].reshape(rows, zs) for q in range(m)],
            axis=1,
        )
        high, low = halves(got)
        both = dot(jnp.concatenate([high, low], axis=0), tzh[...])
        full = both[:rows] + both[rows:] + dot(high, tzl[...])
        at = slice(starts[k] * yc, starts[k] * yc + rows)
        out[at, :] = full * f[at, :]

    for k in range(pieces):
        got_rows(k)
        for which, begun in ((inner_high, begun_high), (inner_low, begun_low)):
            steps = steps_from(k + begun)
            if steps:

                @pl.when(which)
                def _():
                    crosses(steps)

        transform_y(k)
        send_cols(k)
        if k >= lag:
            got_cols(k - lag)
            transform_z(k - lag)
    def sent_all():
        @pl.when(inner)
        def _():
            pltpu.make_async_copy(pass_on, pass_on, send_r).wait()

        sent = s.at[pl.ds(0, (n - 1) * x_share)]
        pltpu.make_async_copy(sent, sent, send_r).wait()

    def sent_cols():
        sent = y.at[pl.ds(0, (m - 1) * x_share)]
        pltpu.make_async_copy(sent, sent, send_c).wait()

    for k in range(pieces - lag, pieces):
        if k == pieces - 1:
            out[last_rows, :] = (out[last_rows, :] + half_z(1 - side, m // 2, k)) * f[last_rows, :]
            break
        if k == max(pieces - 2, pieces - lag):
            sent_all()
            out[last_rows, :] = half_z(side, m // 2 - 1, pieces)

            @pl.when(jnp.logical_and(low, outer))
            def _():
                for at in range(half, tiers):
                    wait_up(at)

        got_cols(k)
        transform_z(k)
    sent_cols()


def per_device(n, m, tracer, symbol_x, symbol_y, symbol_z):
    depth, ys, zs = tracer.shape
    height, length = ys * n, zs * m
    x_share, yc = depth // n, height // m
    sizes = piece_sizes(x_share)
    pieces = len(sizes)
    starts = [sum(sizes[:k]) for k in range(pieces)]
    block = min(height, 128)

    groups = [(0, 1)]
    while sum(groups[-1]) < pieces:
        first = sum(groups[-1])
        count = 1
        while first + count < pieces and n * sum(sizes[first : first + count + 1]) <= 128:
            count += 1
        groups.append((first, count))
    share = np.arange(depth).reshape(n, x_share)
    order = [share[:, a : a + e].reshape(-1) for a, e in zip(starts, sizes)]
    high, low = table_halves(depth)
    tab_x = []
    for first, count in groups:
        rows = np.concatenate(order[first : first + count])
        tab_x.append(left_table(high[rows], low[rows]))
    tab_x = np.concatenate(tab_x)
    high, low = table_halves(height)
    tab_y = [left_table(high[b : b + block], low[b : b + block]) for b in range(0, height, block)]
    tab_y = np.concatenate(tab_y)
    tab_zh, tab_zl = table_halves(length)

    anywhere = pl.BlockSpec(memory_space=pl.ANY)
    dma = pltpu.SemaphoreType.DMA
    regular = pltpu.SemaphoreType.REGULAR
    out = pl.pallas_call(
        functools.partial(kernel, n, m, sizes, groups, block),
        out_shape=pltpu.VMEM((x_share * yc, length), F32),
        in_specs=[anywhere] * 8,
        out_specs=pl.BlockSpec(memory_space=pltpu.VMEM),
        scratch_shapes=[
            pltpu.VMEM((depth, ys, zs), F32),
            pltpu.VMEM((depth, ys, zs), F32),
            pltpu.VMEM((x_share, height, zs), F32),
            pltpu.VMEM((m * x_share, yc, zs), F32),
            pltpu.VMEM((m * x_share, yc, zs), F32),
            pltpu.VMEM((x_share * yc, length), F32),
            pltpu.VMEM((n // 2 * x_share, ys, zs), F32),
            pltpu.VMEM(tab_x.shape, BF16),
            pltpu.VMEM(tab_y.shape, BF16),
            pltpu.VMEM(tab_zh.shape, BF16),
            pltpu.VMEM(tab_zl.shape, BF16),
            pltpu.VMEM((depth, 128), F32),
            pltpu.VMEM((height, 128), F32),
            pltpu.VMEM((1, depth), F32),
            pltpu.VMEM((1, height), F32),
            pltpu.VMEM((1, length), F32),
            dma((2 + CUTS,)),
            dma,
            dma((pieces,)),
            dma,
            dma((pieces + 1,)),
            dma((pieces,)),
            regular((n // 2,)),
            regular,
            regular,
        ],
        compiler_params=pltpu.CompilerParams(
            collective_id=0,
            has_side_effects=True,
            vmem_limit_bytes=(58 << 20) - 12 * x_share * yc * length,
        ),
    )(
        tracer,
        jnp.asarray(tab_x),
        jnp.asarray(tab_y),
        jnp.asarray(tab_zh),
        jnp.asarray(tab_zl),
        symbol_x[None],
        symbol_y[None],
        symbol_z[None],
    )
    return out.reshape(x_share, yc, length)


def solution(mesh):
    in_specs = (P(None, "row", "col"), P(), P(), P())
    out_specs = P("row", "col", None)
    body = functools.partial(per_device, mesh.shape["row"], mesh.shape["col"])
    return jax.shard_map(
        body, mesh=mesh, in_specs=in_specs, out_specs=out_specs, check_vma=False
    )
```

```python
import functools

import jax
import jax.numpy as jnp
import ml_dtypes
import numpy as np
from jax import lax
from jax.experimental import pallas as pl
from jax.experimental.pallas import tpu as pltpu
from jax.sharding import PartitionSpec as P

MESH = pl.DeviceIdType.MESH
F32 = jnp.float32
BF16 = jnp.bfloat16
PIECES = 8
LEAD = 3
OWN = 7
OWN_B = 3
BEGUN = 6
BEGUN_LOW = 7
LAG = 6
CUTS = 2
NEAR_LAG = 5


def table_halves(count):
    rank = np.arange(1, count + 1)
    turns = np.outer(rank, rank) % (2 * count + 2)
    table = np.sin(np.pi / (count + 1) * turns) * np.sqrt(2.0 / (count + 1))
    high = table.astype(ml_dtypes.bfloat16)
    low = (table - high.astype(np.float64)).astype(ml_dtypes.bfloat16)
    return high, low


def left_table(high, low):
    return np.concatenate(
        [np.concatenate([high, high], axis=1), np.concatenate([low, 0 * low], axis=1)]
    )


def halves(values):
    high = values.astype(BF16)
    return high, (values - high.astype(F32)).astype(BF16)


def dot(a, b):
    return jnp.dot(a, b, preferred_element_type=F32)


def from_left(table, values):
    rows = table.shape[0] // 2
    both = dot(table, jnp.concatenate(halves(values), axis=0))
    return both[:rows] + both[rows:]


def piece_sizes(share):
    size = max(1, share // PIECES)
    sizes = []
    left = share
    while left:
        now = size if 4 * left > share else max(1, size // 2)
        sizes.append(min(now, left))
        left -= sizes[-1]
    return sizes


def kernel(
    n, m, sizes, groups, block,
    field, tab_x, tab_y, tab_zh, tab_zl, sx, sy, sz, out,
    d, s, r, y, c, f, pass_on, tx, ty, tzh, tzl, colx, coly, vx, vy, vz,
    in_sem, send_r, recv_r, send_c, recv_c, recv_p, up_r, up_c, up_e,
):
    pieces = len(sizes)
    starts = [sum(sizes[:k]) for k in range(pieces)]
    lag, lead = min(LAG, pieces), min(LEAD, pieces - 1)
    me_r, me_c = lax.axis_index("row"), lax.axis_index("col")
    depth, ys, zs = d.shape
    yc = y.shape[1]
    cut = ys // CUTS
    fields = [pl.ds(i * cut, cut) for i in range(CUTS)]
    fields = [
        pltpu.make_async_copy(field.at[:, at, :], d.at[:, at, :], in_sem.at[2 + i])
        for i, at in enumerate(fields)
    ]
    loads = [(tab_x, tx, 0), (tab_y, ty, 1), (tab_zh, tzh, 1), (tab_zl, tzl, 1)]
    loads += [(sx, vx, 1), (sy, vy, 1), (sz, vz, 1)]
    loads = [pltpu.make_async_copy(a, b, in_sem.at[i]) for a, b, i in loads]

    for load in fields + loads:
        load.start()

    odd = lax.rem(me_r, 2)
    tier = lax.div(me_r, 2)
    tiers = n // 2
    barrier = pltpu.get_barrier_semaphore()
    flip = 1 if m % 2 == 0 else 0
    place = lambda at: at ^ flip

    def greet_row(to, _):
        @pl.when(jnp.logical_or(odd == 0, lax.rem(to, 2) == 1))
        def _():
            pl.semaphore_signal(barrier, inc=1, device_id={"row": to}, device_id_type=MESH)

        return 0

    def greet_col(at, _):
        pl.semaphore_signal(barrier, inc=1, device_id={"col": place(at)}, device_id_type=MESH)
        return 0

    lax.fori_loop(me_r + 1, n, greet_row, 0)
    lax.fori_loop(place(me_c) + 1, m, greet_col, 0)
    earlier = jnp.where(odd == 1, me_r, tier) + place(me_c)

    @pl.when(earlier > 0)
    def _():
        pl.semaphore_wait(barrier, earlier)

    @pl.when(odd == 1)
    def _():
        def answer(to, _):
            pl.semaphore_signal(
                up_r.at[tier], inc=1, device_id={"row": to}, device_id_type=MESH
            )
            return 0

        lax.fori_loop(0, me_r, answer, 0)

    @pl.when(me_r == 2 * (tiers // 2))
    def _():
        for at in range(tiers // 4, tiers // 2):
            pl.semaphore_signal(up_e, inc=1, device_id={"row": 2 * at}, device_id_type=MESH)

    def answer_col(at, _):
        pl.semaphore_signal(up_c, inc=1, device_id={"col": place(at)}, device_id_type=MESH)
        return 0

    lax.fori_loop(0, place(me_c), answer_col, 0)

    loads[0].wait()
    lanes = d.reshape(depth * ys, zs)
    modes = s.reshape(s.shape[0] * ys, zs)

    def transform_x(first, count, after=None):
        begin = n * starts[first]
        rows = n * sum(sizes[first : first + count])
        table = tx[2 * begin : 2 * (begin + rows)]

        def pair(i, _):
            got = jnp.concatenate(
                [lanes[pl.ds(2 * i + h, depth, stride=ys), :] for h in range(2)], axis=1
            )
            got = from_left(table, got)
            for h in range(2):
                modes[pl.ds(begin * ys + 2 * i + h, rows, stride=ys), :] = got[
                    :, h * zs : (h + 1) * zs
                ]
            return 0

        for i in range(CUTS):
            if first == 0:
                fields[i].wait()
            lax.fori_loop(i * cut // 2, (i + 1) * cut // 2, pair, 0, unroll=True)
            if after is not None:
                after(i)

    def rows_of(at):
        return pl.ds(pl.multiple_of(at * ys, ys), ys)

    def send_row(k, to, part=0, parts=1):
        each, some = sizes[k], ys // parts
        into = pl.ds(pl.multiple_of(me_r * ys + part * some, some), some)
        pltpu.make_async_remote_copy(
            src_ref=s.at[pl.ds(n * starts[k] + to * each, each), pl.ds(part * some, some), :],
            dst_ref=r.at[pl.ds(starts[k], each), into, :],
            send_sem=send_r,
            recv_sem=recv_r.at[k],
            device_id={"row": to},
            device_id_type=MESH,
        ).start()

    def keep_row(k):
        each = sizes[k]
        r[pl.ds(starts[k], each), rows_of(me_r), :] = s[pl.ds(n * starts[k] + me_r * each, each)]

    def wait_up(at):
        pl.semaphore_wait(up_r.at[at], 1)

    half, step_out = tiers // 2, tiers // 4
    high = tier >= half
    low = jnp.logical_not(high)
    outer = jnp.logical_or(tier < step_out, tier >= tiers - step_out)
    inner = jnp.logical_not(outer)
    far, near = jnp.where(high, 0, half), jnp.where(high, half, 0)
    behind = jnp.where(high, me_r + 2 * step_out, me_r - 2 * step_out)
    ahead = jnp.where(high, me_r - 2 * step_out, me_r + 2 * step_out)
    every, near_lag = range(pieces), min(NEAR_LAG, pieces)

    def send_tier(k, at, other):
        send_row(k, 2 * at + (odd ^ other))

    def send_tiers(ks, begin, end, wait=False):
        def one(at, _):
            if wait:
                wait_up(at)
            for k in ks:
                for other in range(2):
                    send_row(k, 2 * at + other)
            return 0

        lax.fori_loop(begin, end, one, 0)

    def hand_on(k):
        each = sizes[k]
        pltpu.make_async_remote_copy(
            src_ref=s.at[pl.ds(n * starts[k] + 2 * far * each, n // 2 * each)],
            dst_ref=pass_on.at[pl.ds(n // 2 * starts[k], n // 2 * each)],
            send_sem=send_r,
            recv_sem=recv_p.at[k],
            device_id={"row": ahead},
            device_id_type=MESH,
        ).start()

    def got_pass(k):
        waited = pass_on.at[pl.ds(n // 2 * starts[k], n // 2 * sizes[k])]
        pltpu.make_async_copy(waited, waited, recv_p.at[k]).wait()

    def pass_rows(k, begin, end):
        each = sizes[k]

        def one(to, _):
            pltpu.make_async_remote_copy(
                src_ref=pass_on.at[pl.ds(n // 2 * starts[k] + (to - 2 * far) * each, each)],
                dst_ref=r.at[pl.ds(starts[k], each), rows_of(behind), :],
                send_sem=send_r,
                recv_sem=recv_r.at[k],
                device_id={"row": to},
                device_id_type=MESH,
            ).start()
            return 0

        lax.fori_loop(begin, end, one, 0)

    def own_rows(k, begin, end):
        def one(to, _):
            send_row(k, to)
            return 0

        lax.fori_loop(begin, end, one, 0)

    def hear_peer():
        @pl.when(odd == 0)
        def _():
            wait_up(tier)

    def start_far(part):
        def same(at, _):
            send_row(0, 2 * at + odd, part, CUTS)
            return 0

        lax.fori_loop(0, half, same, 0)

        if part == CUTS - 1:
            hear_peer()

            def other(at, _):
                send_tier(0, at, 1)
                return 0

            lax.fori_loop(0, half, other, 0)

    def start_low():
        @pl.when(odd == 0)
        def _():
            pl.semaphore_wait(up_e, 1)
            send_tier(0, half, 0)

        @pl.when(odd == 1)
        def _():
            wait_up(half)
            send_tier(0, half, 0)
            send_tier(0, half, 1)

    def send_peer():
        for k in every:
            send_tier(k, tier, 1)

    begin, turn, end = 2 * far, jnp.where(high, 1, n), jnp.where(high, n // 2, n)

    def by_core(act):
        for core, own in enumerate((OWN, OWN_B)):

            @pl.when(lax.rem(me_c, 2) == core)
            def _():
                act(min(own, pieces))

    def cross(step, own):
        def part(step, begin, end):
            if 0 <= step < pieces:
                pass_rows(step, begin, end)
            for k in range(own, pieces):
                if k - max(1, 2 * own - 1 - k) == step:
                    own_rows(k, begin, end)

        if step < pieces:
            got_pass(step)
            part(step, begin, turn)
        if 0 <= step - lead:
            part(step - lead, turn, end)

    inner_high, inner_low = jnp.logical_and(high, inner), jnp.logical_and(low, inner)
    begun_high, begun_low = min(BEGUN, pieces), min(BEGUN_LOW, pieces)

    def first_sends(part):
        @pl.when(inner_high)
        def _():
            start_far(part)

        if part == CUTS - 1:

            @pl.when(inner_low)
            def _():
                start_low()

            @pl.when(jnp.logical_and(high, outer))
            def _():
                hand_on(0)

    for at, (first, count) in enumerate(groups):
        transform_x(first, count, None if at else first_sends)

    @pl.when(jnp.logical_and(high, inner))
    def _():
        by_core(lambda own: [send_tiers([k], far, far + half) for k in range(1, own)])
        send_peer()
        send_tiers(every, tier + 1, tiers, wait=True)

    @pl.when(inner_low)
    def _():
        def more(own):
            for k in range(1, own):
                send_tier(k, half, 0)

        by_core(more)
        hear_peer()
        send_tiers(every, 0, tier)
        send_peer()

        @pl.when(odd == 0)
        def _():
            wait_up(half)
            send_tier(0, half, 1)

        def others(own):
            for k in range(1, own):
                send_tier(k, half, 1)

        by_core(others)
        for at in range(half + 1, tiers):
            wait_up(at)
            by_core(lambda own: send_tiers(range(own), at, at + 1))

    @pl.when(jnp.logical_and(high, outer))
    def _():
        hear_peer()
        for k in range(pieces + near_lag):
            if 0 < k < pieces:
                hand_on(k)
            if k >= near_lag:
                send_tiers([k - near_lag], half, tier)
        send_peer()
        send_tiers(every, tier + 1, tiers, wait=True)

    @pl.when(jnp.logical_and(low, outer))
    def _():
        hear_peer()
        send_peer()
        send_tiers(every, 0, tier)

        def one(at, _):
            wait_up(at)
            return 0

        lax.fori_loop(tier + 1, half, one, 0)
        for k in range(pieces + near_lag):
            if k < pieces:
                hand_on(k)
            if k >= near_lag:
                send_tiers([k - near_lag], tier + 1, half)

    def crosses(steps):
        by_core(lambda own: [cross(step, own) for step in steps])

    def steps_from(step):
        return [at for at in range(step, pieces + lead) if at == step or step == pieces - 1] * (
            step < pieces
        )

    @pl.when(inner_high)
    def _():
        for step in range(begun_high):
            crosses(steps_from(step))

    @pl.when(inner_low)
    def _():
        for step in range(begun_low):
            crosses(steps_from(step))

    for k in every:
        keep_row(k)

    for load in loads[1:]:
        load.wait()

    def upright(row_ref, into):
        size = row_ref.shape[1]
        here = lax.broadcasted_iota(jnp.int32, (size, size), 0)
        there = lax.broadcasted_iota(jnp.int32, (size, size), 1)
        kept = jnp.where(here == there, row_ref[...], 0.0)
        into[...] = jnp.broadcast_to(jnp.sum(kept, axis=1, keepdims=True), into.shape)

    upright(vx, colx)
    upright(vy, coly)
    x_share = r.shape[0]
    part_y = coly[pl.ds(pl.multiple_of(me_c * yc, yc), yc), :]

    def factor(i, _):
        symbol = part_y + colx[pl.ds(me_r * x_share + i, 1), :]
        for at in range(0, vz.shape[1], 128):
            full = symbol + vz[:, at : at + 128]
            f[pl.ds(pl.multiple_of(i * yc, yc), yc), at : at + 128] = (1.0 - 0.2 * full) / (
                1.0 + 0.2 * full
            )
        return 0

    lax.fori_loop(0, x_share, factor, 0)

    @pl.when(place(me_c) < m - 1)
    def _():
        pl.semaphore_wait(up_c, m - 1 - place(me_c))

    def got_rows(k):
        waited = r.at[pl.ds(starts[k], sizes[k]), pl.ds(0, (n - 1) * ys), :]
        pltpu.make_async_copy(waited, waited, recv_r.at[k]).wait()

    def transform_y(k):
        each, base = sizes[k], m * starts[k]
        got = jnp.concatenate([r[starts[k] + j] for j in range(each)], axis=1)
        for b in range(ty.shape[0] // (2 * block)):
            now = from_left(ty[2 * b * block : 2 * (b + 1) * block], got)
            for q in range(block // yc):
                for j in range(each):
                    y[base + (b * (block // yc) + q) * each + j] = now[
                        q * yc : (q + 1) * yc, j * zs : (j + 1) * zs
                    ]

    def send_cols(k):
        each, base = sizes[k], m * starts[k]

        def one(i, _):
            to = lax.rem(me_c + i, m)
            beside = (lax.div(to, m // 2) == side).astype(jnp.int32) if k == pieces - 1 else 0
            pltpu.make_async_remote_copy(
                src_ref=y.at[pl.ds(base + to * each, each)],
                dst_ref=c.at[pl.ds(base + me_c * each, each)],
                send_sem=send_c,
                recv_sem=recv_c.at[k + beside],
                device_id={"col": to},
                device_id_type=MESH,
            ).start()
            return 0

        lax.fori_loop(1, m, one, 0)
        own = pl.ds(base + me_c * each, each)
        c[own] = y[own]

    def got_cols(k):
        waited = c.at[pl.ds(m * starts[k], (m - 1) * sizes[k])]
        pltpu.make_async_copy(waited, waited, recv_c.at[k]).wait()

    side = lax.div(me_c, m // 2)

    def half_z(at_side, count, sem):
        k = pieces - 1
        each, base = sizes[k], m * starts[k]
        rows, many = each * yc, m // 2 * zs
        if count:
            waited = c.at[pl.ds(base, count * each)]
            pltpu.make_async_copy(waited, waited, recv_c.at[sem]).wait()
        got = [
            c[pl.ds(base + (at_side * (m // 2) + q) * each, each)].reshape(rows, zs)
            for q in range(m // 2)
        ]
        high, low = halves(jnp.concatenate(got, axis=1))
        some = pl.ds(pl.multiple_of(at_side * many, many), many)
        both = dot(jnp.concatenate([high, low], axis=0), tzh[some, :])
        return both[:rows] + both[rows:] + dot(high, tzl[some, :])

    last_rows = slice(starts[pieces - 1] * yc, (starts[pieces - 1] + sizes[pieces - 1]) * yc)

    def transform_z(k):
        each, base = sizes[k], m * starts[k]
        rows = each * yc
        got = jnp.concatenate(
            [c[base + q * each : base + (q + 1) * each].reshape(rows, zs) for q in range(m)],
            axis=1,
        )
        high, low = halves(got)
        both = dot(jnp.concatenate([high, low], axis=0), tzh[...])
        full = both[:rows] + both[rows:] + dot(high, tzl[...])
        at = slice(starts[k] * yc, starts[k] * yc + rows)
        out[at, :] = full * f[at, :]

    for k in range(pieces):
        got_rows(k)
        for which, begun in ((inner_high, begun_high), (inner_low, begun_low)):
            steps = steps_from(k + begun)
            if steps:

                @pl.when(which)
                def _():
                    crosses(steps)

        transform_y(k)
        send_cols(k)
        if k >= lag:
            got_cols(k - lag)
            transform_z(k - lag)
    def sent_all():
        @pl.when(inner)
        def _():
            pltpu.make_async_copy(pass_on, pass_on, send_r).wait()

        sent = s.at[pl.ds(0, (n - 1) * x_share)]
        pltpu.make_async_copy(sent, sent, send_r).wait()

    def sent_cols():
        sent = y.at[pl.ds(0, (m - 1) * x_share)]
        pltpu.make_async_copy(sent, sent, send_c).wait()

    for k in range(pieces - lag, pieces):
        if k == pieces - 1:
            out[last_rows, :] = (out[last_rows, :] + half_z(1 - side, m // 2, k)) * f[last_rows, :]
            break
        if k == max(pieces - 2, pieces - lag):
            sent_all()
            out[last_rows, :] = half_z(side, m // 2 - 1, pieces)

            @pl.when(jnp.logical_and(low, outer))
            def _():
                for at in range(half, tiers):
                    wait_up(at)

        got_cols(k)
        transform_z(k)
    sent_cols()


def per_device(n, m, tracer, symbol_x, symbol_y, symbol_z):
    depth, ys, zs = tracer.shape
    height, length = ys * n, zs * m
    x_share, yc = depth // n, height // m
    sizes = piece_sizes(x_share)
    pieces = len(sizes)
    starts = [sum(sizes[:k]) for k in range(pieces)]
    block = min(height, 128)

    groups = [(0, 1)]
    while sum(groups[-1]) < pieces:
        first = sum(groups[-1])
        count = 1
        while first + count < pieces and n * sum(sizes[first : first + count + 1]) <= 128:
            count += 1
        groups.append((first, count))
    share = np.arange(depth).reshape(n, x_share)
    order = [share[:, a : a + e].reshape(-1) for a, e in zip(starts, sizes)]
    high, low = table_halves(depth)
    tab_x = []
    for first, count in groups:
        rows = np.concatenate(order[first : first + count])
        tab_x.append(left_table(high[rows], low[rows]))
    tab_x = np.concatenate(tab_x)
    high, low = table_halves(height)
    tab_y = [left_table(high[b : b + block], low[b : b + block]) for b in range(0, height, block)]
    tab_y = np.concatenate(tab_y)
    tab_zh, tab_zl = table_halves(length)

    anywhere = pl.BlockSpec(memory_space=pl.ANY)
    dma = pltpu.SemaphoreType.DMA
    regular = pltpu.SemaphoreType.REGULAR
    out = pl.pallas_call(
        functools.partial(kernel, n, m, sizes, groups, block),
        out_shape=pltpu.VMEM((x_share * yc, length), F32),
        in_specs=[anywhere] * 8,
        out_specs=pl.BlockSpec(memory_space=pltpu.VMEM),
        scratch_shapes=[
            pltpu.VMEM((depth, ys, zs), F32),
            pltpu.VMEM((depth, ys, zs), F32),
            pltpu.VMEM((x_share, height, zs), F32),
            pltpu.VMEM((m * x_share, yc, zs), F32),
            pltpu.VMEM((m * x_share, yc, zs), F32),
            pltpu.VMEM((x_share * yc, length), F32),
            pltpu.VMEM((n // 2 * x_share, ys, zs), F32),
            pltpu.VMEM(tab_x.shape, BF16),
            pltpu.VMEM(tab_y.shape, BF16),
            pltpu.VMEM(tab_zh.shape, BF16),
            pltpu.VMEM(tab_zl.shape, BF16),
            pltpu.VMEM((depth, 128), F32),
            pltpu.VMEM((height, 128), F32),
            pltpu.VMEM((1, depth), F32),
            pltpu.VMEM((1, height), F32),
            pltpu.VMEM((1, length), F32),
            dma((2 + CUTS,)),
            dma,
            dma((pieces,)),
            dma,
            dma((pieces + 1,)),
            dma((pieces,)),
            regular((n // 2,)),
            regular,
            regular,
        ],
        compiler_params=pltpu.CompilerParams(
            collective_id=0,
            has_side_effects=True,
            vmem_limit_bytes=(58 << 20) - 12 * x_share * yc * length,
        ),
    )(
        tracer,
        jnp.asarray(tab_x),
        jnp.asarray(tab_y),
        jnp.asarray(tab_zh),
        jnp.asarray(tab_zl),
        symbol_x[None],
        symbol_y[None],
        symbol_z[None],
    )
    return out.reshape(x_share, yc, length)


def solution(mesh):
    in_specs = (P(None, "row", "col"), P(), P(), P())
    out_specs = P("row", "col", None)
    body = functools.partial(per_device, mesh.shape["row"], mesh.shape["col"])
    return jax.shard_map(
        body, mesh=mesh, in_specs=in_specs, out_specs=out_specs, check_vma=False
    )
```
